32 devices in a mesh: rep: 2 (over x), data: 4 (over z), expert: 4 (over y, core).
Axes of the slice: x: 2, y: 2, z: 4, core: 2. Of those that a mesh axis runs over, the one named last changes fastest.
Arguments:
- x: bfloat16 [128, 512, 1024], P(('rep', 'expert', 'data')), parts along dimension 0
- expert_idx: int32 [128, 512, 8], P(('rep', 'expert', 'data')), parts along dimension 0
- gate: float32 [128, 512, 8], P(('rep', 'expert', 'data')), parts along dimension 0
- attn_gain: float32 [1024], replicated
- w_qkv: bfloat16 [1024, 32, 64], P(('data', 'expert'))
- w_out: bfloat16 [16, 64, 1024], P(None, None, ('data', 'expert'))
- moe_gain: float32 [1024], replicated
- w_gate: bfloat16 [32, 1024, 512], P('expert', 'data')
- w_up: bfloat16 [32, 1024, 512], P('expert', 'data')
- w_down: bfloat16 [32, 512, 1024], P('expert', None, 'data')
Outputs:
- output: bfloat16 [128, 512, 1024], P(('rep', 'expert', 'data')), parts along dimension 0
There are 2 independent parts. The reference program is written for one: setup_inputs(seed, part) draws one part's arguments, and reference() takes and returns one part's arrays. A program takes and returns all parts, laid end to end along the dimension named above; an argument that names none is the same for every part.
All inputs are finite; a program needn't handle non-finite values.
Results may differ from the reference program's by a relative error of at most 0.015028.
Values are sent between devices in bfloat16 or wider.
A program may use at most 1 GiB of HBM per device.

```python
import jax
import jax.numpy as jnp
from jax import lax

MODEL_DIM = 1024
EXPERT_FF = 512
EXPERTS = 32
TOP_K = 8
NUM_HEADS = 16
KV_HEADS = 8
HEAD_DIM = 64
SEQ_LEN = 512
SEQS_DEV = 4
EXPERT_AXIS = 4
DATA_AXIS = 4

TOK_DEV = SEQS_DEV * SEQ_LEN
GROUP_DEVS = EXPERT_AXIS * DATA_AXIS
CAPACITY = 8 * ((5 * TOP_K * TOK_DEV + 32 * EXPERTS - 1) // (32 * EXPERTS))
QKV_HEADS = NUM_HEADS + 2 * KV_HEADS
GROUP_LEN = NUM_HEADS // KV_HEADS
NORM_EPS = 1e-6
ROPE_BASE = 10000.0


def draw_routing(key):
    noise_key, hot_key, perm_key = jax.random.split(key, 3)
    noise = jax.random.randint(noise_key, (GROUP_DEVS, TOK_DEV, EXPERTS), 0, 1 << 20)
    hot_ids = jax.random.randint(hot_key, (GROUP_DEVS,), 0, EXPERTS)
    perm_keys = jax.random.split(perm_key, GROUP_DEVS)
    ranks = jax.vmap(lambda one_key: jax.random.permutation(one_key, TOK_DEV))(perm_keys)
    flagged = ranks < TOK_DEV // 2
    is_hot = jnp.arange(EXPERTS)[None, None, :] == hot_ids[:, None, None]
    score = (noise + jnp.where(flagged[:, :, None] & is_hot, 1 << 21, 0)) * EXPERTS + jnp.arange(EXPERTS)[None, None, :]
    chosen = lax.top_k(score, TOP_K)[1]
    return chosen.astype(jnp.int32).reshape(GROUP_DEVS * SEQS_DEV, SEQ_LEN, TOP_K)


def setup_inputs(seed: int = 0, part: int = 0) -> dict:
    base_key = jax.random.key(seed)
    part_key = jax.random.fold_in(base_key, part)
    x_key, route_key, gate_key = jax.random.split(part_key, 3)
    weight_keys = jax.random.split(jax.random.key(seed + 1), 7)
    num_seqs = GROUP_DEVS * SEQS_DEV
    x = jax.random.normal(x_key, (num_seqs, SEQ_LEN, MODEL_DIM), jnp.float32).astype(jnp.bfloat16)
    expert_idx = draw_routing(route_key)
    gate = jax.random.uniform(gate_key, (num_seqs, SEQ_LEN, TOP_K), jnp.float32, 0.4, 1.6) * TOP_K ** -0.5
    attn_gain = jax.random.uniform(weight_keys[0], (MODEL_DIM,), jnp.float32, 0.5, 1.5)
    w_qkv = (jax.random.normal(weight_keys[1], (MODEL_DIM, QKV_HEADS, HEAD_DIM), jnp.float32) * (1.5 * MODEL_DIM ** -0.5)).astype(jnp.bfloat16)
    w_out = (jax.random.normal(weight_keys[2], (NUM_HEADS, HEAD_DIM, MODEL_DIM), jnp.float32) * (NUM_HEADS * HEAD_DIM) ** -0.5).astype(jnp.bfloat16)
    moe_gain = jax.random.uniform(weight_keys[3], (MODEL_DIM,), jnp.float32, 0.5, 1.5)
    w_gate = (jax.random.normal(weight_keys[4], (EXPERTS, MODEL_DIM, EXPERT_FF), jnp.float32) * MODEL_DIM ** -0.5).astype(jnp.bfloat16)
    w_up = (jax.random.normal(weight_keys[5], (EXPERTS, MODEL_DIM, EXPERT_FF), jnp.float32) * MODEL_DIM ** -0.5).astype(jnp.bfloat16)
    w_down = (jax.random.normal(weight_keys[6], (EXPERTS, EXPERT_FF, MODEL_DIM), jnp.float32) * (2.0 * EXPERT_FF ** -0.5)).astype(jnp.bfloat16)
    return {'x': x, 'expert_idx': expert_idx, 'gate': gate, 'attn_gain': attn_gain, 'w_qkv': w_qkv, 'w_out': w_out, 'moe_gain': moe_gain, 'w_gate': w_gate, 'w_up': w_up, 'w_down': w_down}


def rms_scale(tok_rows, gain):
    rows_f32 = tok_rows.astype(jnp.float32)
    inv_rms = lax.rsqrt(jnp.mean(rows_f32 * rows_f32, axis=-1, keepdims=True) + NORM_EPS)
    return (rows_f32 * inv_rms * gain).astype(jnp.bfloat16)


def apply_rope(head_vals):
    half_dim = HEAD_DIM // 2
    inv_freq = ROPE_BASE ** (-jnp.arange(half_dim, dtype=jnp.float32) * 2.0 / HEAD_DIM)
    angles = jnp.arange(SEQ_LEN, dtype=jnp.float32)[:, None] * inv_freq[None, :]
    cos_b = jnp.cos(angles)[:, None, :]
    sin_b = jnp.sin(angles)[:, None, :]
    vals_f32 = head_vals.astype(jnp.float32)
    low_half = vals_f32[..., :half_dim]
    high_half = vals_f32[..., half_dim:]
    return jnp.concatenate([low_half * cos_b - high_half * sin_b, high_half * cos_b + low_half * sin_b], axis=-1).astype(jnp.bfloat16)


def attend_one(seq_x, attn_gain, w_qkv, w_out):
    normed = rms_scale(seq_x, attn_gain)
    qkv_all = jnp.dot(normed, w_qkv.reshape(MODEL_DIM, QKV_HEADS * HEAD_DIM), preferred_element_type=jnp.float32).astype(jnp.bfloat16).reshape(SEQ_LEN, QKV_HEADS, HEAD_DIM)
    queries = apply_rope(qkv_all[:, :NUM_HEADS]).reshape(SEQ_LEN, KV_HEADS, GROUP_LEN, HEAD_DIM)
    keys_rot = apply_rope(qkv_all[:, NUM_HEADS:NUM_HEADS + KV_HEADS])
    values = qkv_all[:, NUM_HEADS + KV_HEADS:]
    scores = jnp.einsum('lkgd,mkd->kglm', queries.astype(jnp.float32), keys_rot.astype(jnp.float32)) * (HEAD_DIM ** -0.5)
    causal = jnp.arange(SEQ_LEN)[:, None] >= jnp.arange(SEQ_LEN)[None, :]
    attn_probs = jax.nn.softmax(jnp.where(causal, scores, -1e30), axis=-1).astype(jnp.bfloat16)
    mixed = jnp.einsum('kglm,mkd->lkgd', attn_probs.astype(jnp.float32), values.astype(jnp.float32)).astype(jnp.bfloat16)
    attn_proj = jnp.dot(mixed.reshape(SEQ_LEN, NUM_HEADS * HEAD_DIM), w_out.reshape(NUM_HEADS * HEAD_DIM, MODEL_DIM), preferred_element_type=jnp.float32)
    return (seq_x.astype(jnp.float32) + attn_proj).astype(jnp.bfloat16)


def dispatch_target(flat_ids):
    onehot = (flat_ids[:, None] == jnp.arange(EXPERTS)[None, :]).astype(jnp.int32)
    earlier = jnp.cumsum(onehot, axis=0) - onehot
    slot_pos = jnp.sum(earlier * onehot, axis=1)
    return jnp.where(slot_pos < CAPACITY, flat_ids * CAPACITY + slot_pos, EXPERTS * CAPACITY)


def run_expert(operands):
    tok_rows, gate_w, up_w, down_w = operands
    rows_f32 = tok_rows.astype(jnp.float32)
    act_gate = jnp.dot(rows_f32, gate_w.astype(jnp.float32))
    act_up = jnp.dot(rows_f32, up_w.astype(jnp.float32))
    mid_act = (jax.nn.silu(act_gate) * act_up).astype(jnp.bfloat16)
    return jnp.dot(mid_act.astype(jnp.float32), down_w.astype(jnp.float32)).astype(jnp.bfloat16)


def reference(x, expert_idx, gate, attn_gain, w_qkv, w_out, moe_gain, w_gate, w_up, w_down):
    hidden = lax.map(lambda seq_x: attend_one(seq_x, attn_gain, w_qkv, w_out), x)
    hid_dev = hidden.reshape(GROUP_DEVS, TOK_DEV, MODEL_DIM)
    ids_dev = expert_idx.reshape(GROUP_DEVS, TOK_DEV * TOP_K)
    gate_dev = gate.reshape(GROUP_DEVS, TOK_DEV, TOP_K)

    def build_buffer(operands):
        hid_rows, flat_ids = operands
        normed = rms_scale(hid_rows, moe_gain)
        target_rows = dispatch_target(flat_ids)
        filled = jnp.zeros((EXPERTS * CAPACITY + 1, MODEL_DIM), jnp.bfloat16).at[target_rows].set(jnp.repeat(normed, TOP_K, axis=0))
        return filled[:EXPERTS * CAPACITY].reshape(EXPERTS, CAPACITY, MODEL_DIM), target_rows

    buffers, target_all = lax.map(build_buffer, (hid_dev, ids_dev))
    by_expert = jnp.transpose(buffers, (1, 0, 2, 3)).reshape(EXPERTS, GROUP_DEVS * CAPACITY, MODEL_DIM)
    expert_out = lax.map(run_expert, (by_expert, w_gate, w_up, w_down))
    out_dev = jnp.transpose(expert_out.reshape(EXPERTS, GROUP_DEVS, CAPACITY, MODEL_DIM), (1, 0, 2, 3)).reshape(GROUP_DEVS, EXPERTS * CAPACITY, MODEL_DIM)

    def combine(operands):
        hid_rows, out_rows, target_rows, gate_rows = operands
        padded = jnp.concatenate([out_rows, jnp.zeros((1, MODEL_DIM), jnp.bfloat16)], axis=0)
        picked = jnp.take(padded, target_rows, axis=0).reshape(TOK_DEV, TOP_K, MODEL_DIM).astype(jnp.float32)
        total = hid_rows.astype(jnp.float32) + jnp.sum(picked * gate_rows[:, :, None], axis=1)
        return total.astype(jnp.bfloat16)

    result = lax.map(combine, (hid_dev, out_dev, target_all, gate_dev))
    return result.reshape(GROUP_DEVS * SEQS_DEV, SEQ_LEN, MODEL_DIM)
```

```python
import functools

import jax
import jax.numpy as jnp
from jax import lax
from jax.experimental import pallas as pl
from jax.experimental.pallas import tpu as pltpu
from jax.sharding import PartitionSpec as P

NORM_EPS = 1e-6
ROPE_BASE = 10000.0
LANES = 128
VMEM_LIMIT = 64000 * 1024


def capacity_of(tok_dev, top_k, num_experts):
    return 8 * ((5 * top_k * tok_dev + 32 * num_experts - 1) // (32 * num_experts))


def rope_tables(seq_len, head_dim):
    half_dim = head_dim // 2
    inv_freq = ROPE_BASE ** (-jnp.arange(half_dim, dtype=jnp.float32) * 2.0 / head_dim)
    angles = jnp.arange(seq_len, dtype=jnp.float32)[:, None] * inv_freq[None, :]
    cos_b, sin_b = jnp.cos(angles), jnp.sin(angles)
    return jnp.concatenate([cos_b] * 4, axis=1), jnp.concatenate([-sin_b, sin_b] * 2, axis=1)


def route_kernel(capacity, idx_ref, gate_ref, tok_ref, gates_ref, count_ref, slot_scr):
    top_k, tokens = idx_ref.shape
    experts = gates_ref.shape[0]
    expert_id = lax.broadcasted_iota(jnp.int32, (experts, tokens), 0)
    chosen = jnp.zeros((experts, tokens), jnp.float32)
    gates = jnp.zeros((experts, tokens), jnp.float32)
    for k in range(top_k):
        hit = idx_ref[k:k + 1, :] == expert_id
        chosen = chosen + jnp.where(hit, 1.0, 0.0)
        gates = gates + jnp.where(hit, gate_ref[k:k + 1, :], 0.0)
    gates_ref[...] = gates
    blk = 256
    upper = jnp.where(lax.broadcasted_iota(jnp.int32, (blk, blk), 0) < lax.broadcasted_iota(jnp.int32, (blk, blk), 1), 1.0, 0.0).astype(jnp.bfloat16)
    before = jnp.zeros((experts, 1), jnp.float32)
    for b in range(tokens // blk):
        part = chosen[:, b * blk:(b + 1) * blk]
        earlier = jnp.dot(part.astype(jnp.bfloat16), upper, preferred_element_type=jnp.float32) + before
        slot = jnp.where((part > 0.0) & (earlier < capacity), earlier, -1.0)
        slot_scr[:, b * blk:(b + 1) * blk] = slot.astype(jnp.int32)
        before = before + jnp.sum(part, axis=1, keepdims=True)
    count_ref[...] = jnp.broadcast_to(jnp.minimum(before, float(capacity)), count_ref.shape).astype(jnp.int32)
    tok_id = lax.broadcasted_iota(jnp.int32, (8, tokens), 1)
    tok_hi = (tok_id >> 8).astype(jnp.float32)
    tok_lo = (tok_id & 255).astype(jnp.float32)
    row_id = lax.broadcasted_iota(jnp.int32, (8, tokens), 0)
    lane_id = lax.broadcasted_iota(jnp.int32, (LANES, tokens), 0)

    def one(e, carry):
        slot = slot_scr[pl.ds(e, 1), :]
        major = jnp.broadcast_to(slot >> 7, (8, tokens)) == row_id
        left = jnp.concatenate([jnp.where(major, tok_hi, 0.0), jnp.where(major, tok_lo, 0.0)], axis=0).astype(jnp.bfloat16)
        minor = jnp.where((slot & 127) == lane_id, 1.0, 0.0).astype(jnp.bfloat16)
        found = lax.dot_general(left, minor, (((1,), (1,)), ((), ())), preferred_element_type=jnp.float32)
        tok_ref[pl.ds(e, 1)] = ((found[:8] * 256.0 + found[8:]) * 8.0).astype(jnp.int32).reshape(1, 8, LANES)
        return carry

    lax.fori_loop(0, experts, one, 0)


def route(idx_t, gate_t, num_experts, capacity):
    tokens = idx_t.shape[1]
    return pl.pallas_call(
        functools.partial(route_kernel, capacity),
        out_shape=(
            jax.ShapeDtypeStruct((num_experts, 8, LANES), jnp.int32),
            jax.ShapeDtypeStruct((num_experts, tokens), jnp.float32),
            jax.ShapeDtypeStruct((num_experts, LANES), jnp.int32),
        ),
        scratch_shapes=[pltpu.VMEM((num_experts, tokens), jnp.int32)],
        compiler_params=pltpu.CompilerParams(vmem_limit_bytes=VMEM_LIMIT),
        cost_estimate=pl.CostEstimate(flops=10_000_000_000, bytes_accessed=1_000_000, transcendentals=0),
        name="route",
    )(idx_t, gate_t)


def rms(rows_f32, gain):
    inv = lax.rsqrt(jnp.mean(rows_f32 * rows_f32, axis=-1, keepdims=True) + NORM_EPS)
    return (rows_f32 * inv * gain).astype(jnp.bfloat16)


def attn_kernel(x_ref, ag_ref, wqkv_ref, wout_ref, mg_ref, cos_ref, sin_ref, h_ref, z_ref, u_scr, qkv_scr, mix_scr):
    seq, dim = x_ref.shape[1], x_ref.shape[2]
    rb = 256
    for r in range(0, seq, rb):
        u_scr[r:r + rb, :] = rms(x_ref[0, r:r + rb, :].astype(jnp.float32), ag_ref[...])
    nq = dim // LANES
    nk = nq // 2
    nblk = 512

    def proj(n, carry):
        cols = pl.ds(pl.multiple_of(n * nblk, nblk), nblk)
        qkv_scr[:, cols] = jnp.dot(u_scr[...], wqkv_ref[:, cols], preferred_element_type=jnp.float32).astype(jnp.bfloat16)
        return carry

    lax.fori_loop(0, qkv_scr.shape[1] // nblk, proj, 0)
    lane = lax.broadcasted_iota(jnp.int32, (seq, LANES), 1)
    low = (lane & 63) < 32
    left = lane < 64
    left_rb = left[:rb]

    def rope(v):
        partner = jnp.where(low, pltpu.roll(v, LANES - 32, 1), pltpu.roll(v, 32, 1))
        return v * cos_ref[...] + partner * sin_ref[...]

    causal = lax.broadcasted_iota(jnp.int32, (rb, rb), 0) >= lax.broadcasted_iota(jnp.int32, (rb, rb), 1)

    def pair(p, carry):
        kcol = pl.ds(pl.multiple_of(dim + p * LANES, LANES), LANES)
        vcol = pl.ds(pl.multiple_of(dim + nk * LANES + p * LANES, LANES), LANES)
        keys = rope(qkv_scr[:, kcol].astype(jnp.float32))
        keys_sw = pltpu.roll(keys, 64, 1)
        vals = qkv_scr[:, vcol].astype(jnp.float32)
        vals_sw = pltpu.roll(vals, 64, 1)
        for j in range(2):
            first, second = (keys, keys_sw) if j == 0 else (keys_sw, keys)
            kk = jnp.where(left, first, second).astype(jnp.bfloat16)
            first, second = (vals, vals_sw) if j == 0 else (vals_sw, vals)
            vv = jnp.where(left, first, second).astype(jnp.bfloat16)
            qcol = pl.ds(pl.multiple_of((2 * p + j) * LANES, LANES), LANES)
            q = rope(qkv_scr[:, qcol].astype(jnp.float32)) * 0.125
            for r in range(0, seq, rb):
                qr = q[r:r + rb]
                outs = []
                for half in range(2):
                    qh = jnp.where(left_rb if half == 0 else ~left_rb, qr, 0.0).astype(jnp.bfloat16)
                    s = lax.dot_general(qh, kk[:r + rb], (((1,), (1,)), ((), ())), preferred_element_type=jnp.float32)
                    diag = jnp.where(causal, s[:, r:], -1e30)
                    s = diag if r == 0 else jnp.concatenate([s[:, :r], diag], axis=1)
                    e = jnp.exp(s - jnp.max(s, axis=1, keepdims=True))
                    probs = (e * (1.0 / jnp.sum(e, axis=1, keepdims=True))).astype(jnp.bfloat16)
                    outs.append(jnp.dot(probs, vv[:r + rb], preferred_element_type=jnp.float32))
                mix_scr[r:r + rb, qcol] = jnp.where(left_rb, outs[0], outs[1]).astype(jnp.bfloat16)
        return carry

    lax.fori_loop(0, nk, pair, 0)
    for r in range(0, seq, rb):
        proj_out = jnp.dot(mix_scr[r:r + rb, :], wout_ref[...], preferred_element_type=jnp.float32)
        hid = (x_ref[0, r:r + rb, :].astype(jnp.float32) + proj_out).astype(jnp.bfloat16).astype(jnp.float32)
        normed = rms(hid, mg_ref[...]).astype(jnp.float32)
        for c in range(dim // LANES):
            rows = pl.ds(r * 8 + c, rb, stride=8)
            h_ref[rows, :] = hid[:, c * LANES:(c + 1) * LANES]
            z_ref[rows, :] = normed[:, c * LANES:(c + 1) * LANES]


def attention(x, attn_gain, w_qkv, w_out, moe_gain):
    num, seq, dim = x.shape
    cos_t, sin_t = rope_tables(seq, 64)
    whole = lambda *shape: pl.BlockSpec(shape, lambda s: (0,) * len(shape), pipeline_mode=pl.Buffered(1))
    rows_out = jax.ShapeDtypeStruct((num * seq * 8, LANES), jnp.float32)
    return pl.pallas_call(
        attn_kernel,
        grid=(num,),
        in_specs=[pl.BlockSpec((1, seq, dim), lambda s: (s, 0, 0)), whole(1, dim), whole(dim, 2 * dim), whole(dim, dim), whole(1, dim), whole(seq, LANES), whole(seq, LANES)],
        out_specs=[pl.BlockSpec((seq * 8, LANES), lambda s: (s, 0))] * 2,
        out_shape=(rows_out, rows_out),
        scratch_shapes=[pltpu.VMEM((seq, dim), jnp.bfloat16), pltpu.VMEM((seq, 2 * dim), jnp.bfloat16), pltpu.VMEM((seq, dim), jnp.bfloat16)],
        compiler_params=pltpu.CompilerParams(vmem_limit_bytes=VMEM_LIMIT),
        cost_estimate=pl.CostEstimate(flops=60_000_000_000, bytes_accessed=30_000_000, transcendentals=0),
        name="attention",
    )(x, attn_gain.reshape(1, dim), w_qkv, w_out, moe_gain.reshape(1, dim), cos_t, sin_t)


def expert_kernel(last, capacity, ids_ref, count_ref, tok_ref, gates_ref, z_hbm, acc_hbm, w_ref, out_ref, z_scr, acc_scr, rows_scr, in_scr, sem):
    step = pl.program_id(0)
    dim = in_scr.shape[1]
    chunks = dim // LANES

    @pl.when(step == 0)
    def _():
        cz = pltpu.make_async_copy(z_hbm, z_scr, sem.at[0])
        ca = pltpu.make_async_copy(acc_hbm, acc_scr, sem.at[1])
        cz.start()
        ca.start()
        cz.wait()
        ca.wait()

    count = count_ref[ids_ref[step]]
    unroll = 16
    trips = (count + unroll - 1) // unroll

    def take(i, carry):
        base = i * unroll
        for j in range(unroll):
            src = pl.multiple_of(tok_ref[0, 0, base + j], 8)
            rows_scr[pl.ds(pl.multiple_of((base + j) * 8, 8), 8), :] = z_scr[pl.ds(src, 8), :]
        return carry

    lax.fori_loop(0, trips, take, 0)
    for c in range(chunks):
        in_scr[:, c * LANES:(c + 1) * LANES] = rows_scr[pl.ds(c, capacity, stride=8), :].astype(jnp.bfloat16)
    rb = 320
    quarter = w_ref.shape[4]
    for r in range(0, capacity, rb):
        act_g = None
        for q in range(4):
            xq = in_scr[r:r + rb, q * quarter:(q + 1) * quarter]
            pg = jnp.dot(xq, w_ref[0, 0, q, 0], preferred_element_type=jnp.float32)
            pu = jnp.dot(xq, w_ref[0, 0, q, 1], preferred_element_type=jnp.float32)
            act_g, act_u = (pg, pu) if act_g is None else (act_g + pg, act_u + pu)
        mid = (act_g * jax.nn.sigmoid(act_g) * act_u).astype(jnp.bfloat16)
        for q in range(4):
            down = w_ref[0, 0, q, 2]
            o = jnp.dot(mid[:, :quarter], down[:, :quarter], preferred_element_type=jnp.float32) + jnp.dot(mid[:, quarter:], down[:, quarter:], preferred_element_type=jnp.float32)
            o = o.astype(jnp.bfloat16).astype(jnp.float32)
            for c in range(quarter // LANES):
                rows_scr[pl.ds(r * 8 + q * (quarter // LANES) + c, rb, stride=8), :] = o[:, c * LANES:(c + 1) * LANES]

    def put(i, carry):
        base = i * unroll
        spots, sums = [], []
        for j in range(unroll):
            dst = pl.multiple_of(tok_ref[0, 0, base + j], 8)
            gate = gates_ref[0, 0, dst >> 3]
            spots.append(pl.ds(dst, 8))
            sums.append(acc_scr[spots[-1], :] + gate * rows_scr[pl.ds(pl.multiple_of((base + j) * 8, 8), 8), :])
        for j in range(unroll):
            acc_scr[spots[j], :] = sums[j]
        return carry

    full = count // unroll
    lax.fori_loop(0, full, put, 0)

    def put_one(i, carry):
        dst = pl.multiple_of(tok_ref[0, 0, i], 8)
        acc_scr[pl.ds(dst, 8), :] = acc_scr[pl.ds(dst, 8), :] + gates_ref[0, 0, dst >> 3] * rows_scr[pl.ds(pl.multiple_of(i * 8, 8), 8), :]
        return carry

    lax.fori_loop(full * unroll, count, put_one, 0)

    @pl.when(step == pl.num_programs(0) - 1)
    def _():
        if last:
            tokens = out_ref.shape[0]
            tb = 512
            for t in range(0, tokens, tb):
                for c in range(chunks):
                    out_ref[t:t + tb, c * LANES:(c + 1) * LANES] = acc_scr[pl.ds(t * 8 + c, tb, stride=8), :].astype(jnp.bfloat16)
        else:
            co = pltpu.make_async_copy(acc_scr, out_ref, sem.at[0])
            co.start()
            co.wait()


def experts(ids, count, tok, gates, z, acc, w, capacity, last):
    steps = ids.shape[0]
    tokens = gates.shape[2]
    dim = 8 * LANES
    if last:
        out_shape, out_spec = jax.ShapeDtypeStruct((tokens, dim), jnp.bfloat16), pl.BlockSpec((tokens, dim), lambda s, i, n: (0, 0), pipeline_mode=pl.Buffered(1))
    else:
        out_shape, out_spec = jax.ShapeDtypeStruct(acc.shape, jnp.float32), pl.BlockSpec(memory_space=pl.ANY)
    n_pos = w.shape[1]
    grid_spec = pltpu.PrefetchScalarGridSpec(
        num_scalar_prefetch=2,
        grid=(steps,),
        in_specs=[
            pl.BlockSpec((1, 1, tok.shape[2]), lambda s, i, n: (i[s], 0, 0), memory_space=pltpu.SMEM),
            pl.BlockSpec((1, 1, tokens), lambda s, i, n: (i[s], 0, 0), memory_space=pltpu.SMEM),
            pl.BlockSpec(memory_space=pl.ANY),
            pl.BlockSpec(memory_space=pl.ANY),
            pl.BlockSpec((1, 1) + w.shape[2:], lambda s, i, n: (s // n_pos, s % n_pos, 0, 0, 0, 0)),
        ],
        out_specs=out_spec,
        scratch_shapes=[
            pltpu.VMEM((tokens * 8, LANES), jnp.float32),
            pltpu.VMEM((tokens * 8, LANES), jnp.float32),
            pltpu.VMEM((capacity * 8, LANES), jnp.float32),
            pltpu.VMEM((capacity, dim), jnp.bfloat16),
            pltpu.SemaphoreType.DMA((2,)),
        ],
    )
    return pl.pallas_call(
        functools.partial(expert_kernel, last, capacity),
        grid_spec=grid_spec,
        out_shape=out_shape,
        input_output_aliases={} if last else {5: 0},
        compiler_params=pltpu.CompilerParams(vmem_limit_bytes=VMEM_LIMIT),
        cost_estimate=pl.CostEstimate(flops=5_000_000_000 * steps, bytes_accessed=3_500_000 * steps, transcendentals=0),
        name="experts",
    )(ids, count, tok, gates, z, acc, w)


def pack(gate_part, up_part, down_part):
    half = down_part.shape[1] // 2
    down = jnp.concatenate([down_part[:, :half], down_part[:, half:]], axis=2)
    return jnp.stack([gate_part, up_part, down], axis=1)


def solution(mesh):
    tok_spec = P(('rep', 'expert', 'data'), None, None)
    group_axes = ('data', 'expert')
    n_exp, n_rep = mesh.shape['expert'], mesh.shape['rep']

    def local_step(x, idx, gate, attn_gain, qkv_part, out_part, moe_gain, gate_part, up_part, down_part):
        num_seqs, seq_len, dim = x.shape
        tokens = num_seqs * seq_len
        top_k = idx.shape[-1]
        loc = gate_part.shape[0]
        num_experts = loc * n_exp
        capacity = capacity_of(tokens, top_k, num_experts)
        w_qkv = lax.all_gather(qkv_part.reshape(qkv_part.shape[0], -1), group_axes, axis=0, tiled=True)
        w_out = lax.all_gather(out_part.reshape(-1, out_part.shape[2]), group_axes, axis=1, tiled=True)
        rep = lax.axis_index('rep')
        packed = pack(gate_part, up_part, down_part)
        chunks = loc // n_rep
        gathered = []
        for c in range(chunks):
            mine = lax.dynamic_index_in_dim(packed, c * n_rep + rep, 0, keepdims=False)
            whole = lax.all_gather(mine, ('rep', 'expert', 'data'), axis=0, tiled=False)
            gathered.append(whole.reshape((n_rep, n_exp, mesh.shape['data']) + mine.shape))
        tok, gates, count = route(idx.reshape(tokens, top_k).T, gate.reshape(tokens, top_k).T, num_experts, capacity)
        tok = tok.reshape(num_experts, 1, 8 * LANES)
        gates = gates.reshape(num_experts, 1, tokens)
        count = count[:, 0]
        acc, z = attention(x, attn_gain, w_qkv, w_out, moe_gain)
        for c in range(chunks):
            ids = jnp.asarray([e * loc + c * n_rep + r for r in range(n_rep) for e in range(n_exp)], jnp.int32)
            acc = experts(ids, count, tok, gates, z, acc, gathered[c], capacity, c == chunks - 1)
        return acc.reshape(num_seqs, seq_len, dim)

    in_specs = (tok_spec, tok_spec, tok_spec, P(None), P(group_axes, None, None), P(None, None, group_axes), P(None), P('expert', 'data', None), P('expert', 'data', None), P('expert', None, 'data'))
    return jax.shard_map(local_step, mesh=mesh, in_specs=in_specs, out_specs=tok_spec, check_vma=False)
```
